32 devices in a mesh: rep: 4 (over x, y), dp: 8 (over z, core).
Axes of the slice: x: 2, y: 2, z: 4, core: 2. Of those that a mesh axis runs over, the one named last changes fastest.
Arguments:
- a: bfloat16 [32, 4, 8192, 1024], P(('rep', 'dp')), parts along dimension 0
- g: bfloat16 [32, 4, 8192, 2816], P(('rep', 'dp')), parts along dimension 0
Outputs:
- output: bfloat16 [16, 1024, 2816], P('rep'), parts along dimension 0
There are 4 independent parts. The reference program is written for one: setup_inputs(seed, part) draws one part's arguments, and reference() takes and returns one part's arrays. A program takes and returns all parts, laid end to end along the dimension named above; each array names one.
All inputs are finite; a program needn't handle non-finite values.
Results may differ from the reference program's by a relative error of at most 0.012.
Values are sent between devices in bfloat16 or wider.
A program may use at most 2 GiB of HBM per device.

```python
import jax
import jax.numpy as jnp
from jax import lax

DEVICES = 8
MATRICES = 4
TOKENS = 8192
D = 1024
FF = 2816


def setup_inputs(seed: int = 0, part: int = 0) -> dict:
    ka, kg, ks = (jax.random.fold_in(k, part) for k in jax.random.split(jax.random.key(seed), 3))
    size = 2.0 ** jax.random.uniform(ks, (DEVICES, MATRICES, 1, 1), jnp.float32, -1.0, 1.0)
    a = jax.random.normal(ka, (DEVICES, MATRICES, TOKENS, D), jnp.float32)
    g = size * jax.random.normal(kg, (DEVICES, MATRICES, TOKENS, FF), jnp.float32) * (DEVICES * TOKENS) ** -0.5
    return {"a": a.astype(jnp.bfloat16), "g": g.astype(jnp.bfloat16)}


def reference(a, g):
    def take(so_far, one):
        return so_far + jnp.einsum("ntd,ntf->ndf", *one, preferred_element_type=jnp.float32), None

    return lax.scan(take, jnp.zeros((MATRICES, D, FF), jnp.float32), (a, g))[0].astype(jnp.bfloat16)
```

```python
import functools

import jax
import jax.numpy as jnp
from jax import lax
from jax.experimental import pallas as pl
from jax.experimental.pallas import tpu as pltpu
from jax.sharding import PartitionSpec as P

MESH = pl.DeviceIdType.MESH
BF16, F32 = jnp.bfloat16, jnp.float32

T, D, F, NM = 8192, 1024, 2816, 4
TM, TN, H = 512, 256, 256
KB = 512
NA = 4
KS = T // 256
R, J = D // TM, F // TN
SM = R * J
S = NM * SM
NB = T // KB
NR = 16
NP = 8
NS = 4
LX, LE, LM, LF, LG, LH = 2, 4, 6, 8, 10, 12


def kernel(a, g, o, at0, at1, gbuf, araw, pb, xs, xr, es, er, mr, fs, asem, gsem,
           xss, xrs, ess, ers, mrs, fss, frs, gss, hrs):
    me = lax.axis_index("dp")
    z, c = me // 2, lax.rem(me, 2)
    end = (z == 0) | (z == 3)
    mid = (z == 1) | (z == 2)
    ats = (at0, at1)

    def dev(zz, cc):
        return {"dp": zz * 2 + cc}

    z_mid = jnp.where(z == 0, 1, 2)
    z_end = jnp.where(z == 1, 0, 3)
    z_other = jnp.where(z == 1, 2, 1)
    inward = jnp.where(end, z_mid, z_other)
    sibling = dev(z, 1 - c)

    def acopy(n, b):
        return pltpu.make_async_copy(a.at[n, pl.ds(b * KB, KB), :], araw.at[lax.rem(b, NA)], asem.at[lax.rem(b, NA)])

    def gcopy(u):
        cols = pl.ds(pl.multiple_of(lax.rem(u, J) * TN, TN), TN)
        return pltpu.make_async_copy(g.at[u // J, :, cols], gbuf.at[lax.rem(u, 2)], gsem.at[lax.rem(u, 2)])

    def turn(dst, b, i):
        ti, di = i % (KB // 256), i // (KB // 256)
        dst[b * (KB // 256) + ti, pl.ds(di * 256, 256), :] = araw[
            lax.rem(b, NA), pl.ds(ti * 256, 256), pl.ds(di * 256, 256)].T

    def place(u, h):
        q = lax.rem(u, SM)
        rows = pl.ds(pl.multiple_of(lax.rem(q, R) * TM + h * H, H), H)
        return o.at[u // SM, rows, pl.ds(pl.multiple_of(q // R * TN, TN), TN)]

    def remote(src, dst, send, recv, device):
        return pltpu.make_async_remote_copy(
            src_ref=src, dst_ref=dst, send_sem=send, recv_sem=recv, device_id=device, device_id_type=MESH)

    def xcopy(u):
        i, k = lax.rem(u, NR), lax.rem(u, NS)
        return remote(xs.at[k], xr.at[i], xss.at[k], xrs.at[i], sibling)

    def ecopy(u):
        i, k = lax.rem(u, NR), lax.rem(u, NS)
        return remote(es.at[k], er.at[i], ess.at[k], ers.at[i], dev(inward, c))

    def mcopy(u):
        i, k = lax.rem(u, NR), lax.rem(u, NS)
        return remote(es.at[k], mr.at[i], ess.at[k], mrs.at[i], dev(inward, c))

    def fcopies(u):
        i, k = lax.rem(u, NR), lax.rem(u, NS)
        return (
            remote(fs.at[k], place(u, c), fss.at[k, 0], frs.at[i], dev(z_end, c)),
            remote(fs.at[k], place(u, c), fss.at[k, 1], frs.at[i], dev(z_other, c)),
            remote(fs.at[k], place(u, c), fss.at[k, 2], hrs.at[i], sibling),
        )

    def fkeep(u):
        k = lax.rem(u, NS)
        return pltpu.make_async_copy(fs.at[k], place(u, c), fss.at[k, 3])

    def onward(u):
        i, k = lax.rem(u, NR), lax.rem(u, NS)
        return remote(place(u, c), place(u, c), gss.at[k, 0], frs.at[i], dev(z_end, c))

    def across(u):
        i, k = lax.rem(u, NR), lax.rem(u, NS)
        return remote(place(u, c), place(u, c), gss.at[k, 1], hrs.at[i], sibling)

    def mine(u):
        return z == 1 + lax.rem(u, 2)

    def chip_sum(u):
        return pb[lax.rem(u, NP), pl.ds(pl.multiple_of(c * H, H), H), :] + xr[lax.rem(u, NR)].astype(F32)

    def live(u, top=S):
        return (u >= 0) & (u < top)

    def stage_x(u):
        @pl.when(live(u - NS))
        def _():
            xcopy(u - NS).wait_send()

        @pl.when(live(u))
        def _():
            xs[lax.rem(u, NS)] = pb[lax.rem(u, NP), pl.ds(pl.multiple_of((1 - c) * H, H), H), :].astype(BF16)
            xcopy(u).start()

    def stage_end(u):
        @pl.when(end & live(u - NS))
        def _():
            ecopy(u - NS).wait_send()

        @pl.when(end & live(u))
        def _():
            xcopy(u).wait_recv()
            es[lax.rem(u, NS)] = chip_sum(u).astype(BF16)
            ecopy(u).start()

    def stage_pass(u):
        pass_on = mid & ~mine(u)

        @pl.when(pass_on & live(u - NS))
        def _():
            mcopy(u - NS).wait_send()

        @pl.when(pass_on & live(u))
        def _():
            xcopy(u).wait_recv()
            ecopy(u).wait_recv()
            es[lax.rem(u, NS)] = (chip_sum(u) + er[lax.rem(u, NR)].astype(F32)).astype(BF16)
            mcopy(u).start()

    def stage_own(u):
        @pl.when(mid & mine(u) & live(u - NS))
        def _():
            for copy in fcopies(u - NS):
                copy.wait_send()
            fkeep(u - NS).wait()

        @pl.when(mid & mine(u) & live(u))
        def _():
            xcopy(u).wait_recv()
            ecopy(u).wait_recv()
            mcopy(u).wait_recv()
            i = lax.rem(u, NR)
            fs[lax.rem(u, NS)] = (chip_sum(u) + er[i].astype(F32) + mr[i].astype(F32)).astype(BF16)
            for copy in fcopies(u):
                copy.start()
            fkeep(u).start()

    def stage_forward(u):
        pass_on = mid & ~mine(u)

        @pl.when(pass_on & live(u - NS))
        def _():
            onward(u - NS).wait_send()
            across(u - NS).wait_send()

        @pl.when(pass_on & live(u))
        def _():
            onward(u).wait_recv()
            onward(u).start()
            across(u).start()

    def stage_last(u):
        @pl.when(end & live(u - NS))
        def _():
            across(u - NS).wait_send()

        @pl.when(end & live(u))
        def _():
            onward(u).wait_recv()
            across(u).start()

    def stage_home(u):
        @pl.when(live(u))
        def _():
            across(u).wait_recv()

    def serve(s):
        stage_end(s - LX)
        stage_own(s - LM)
        stage_forward(s - LF)
        stage_pass(s - LE)
        stage_last(s - LG)
        stage_home(s - LH)

    barrier = pltpu.get_barrier_semaphore()
    pl.semaphore_signal(barrier, inc=1, device_id=sibling, device_id_type=MESH)

    @pl.when(z > 0)
    def _():
        pl.semaphore_signal(barrier, inc=1, device_id=dev(z - 1, c), device_id_type=MESH)

    @pl.when(z < 3)
    def _():
        pl.semaphore_signal(barrier, inc=1, device_id=dev(z + 1, c), device_id_type=MESH)

    for b in range(NA):
        acopy(0, b).start()
    gcopy(0).start()

    def first(b, _):
        acopy(0, b).wait()
        for i in range(8):
            turn(at0, b, i)

        @pl.when(b + NA < NB)
        def _():
            acopy(0, b + NA).start()
        return 0

    lax.fori_loop(0, NB, first, 0)
    for b in range(NA - 1):
        acopy(1, b).start()

    @pl.when(end)
    def _():
        pl.semaphore_wait(barrier, 2)

    @pl.when(mid)
    def _():
        pl.semaphore_wait(barrier, 3)

    for n in range(NM):
        now, later = ats[n % 2], ats[(n + 1) % 2]

        def step(q, _, n=n, now=now, later=later):
            s = n * SM + q
            j, r = q // R, lax.rem(q, R)
            u = n * J + j

            @pl.when(r == 0)
            def _():
                gcopy(u).wait()

                @pl.when(u + 1 < NM * J)
                def _():
                    gcopy(u + 1).start()

            b = jnp.minimum(q, NB - 1)
            if n < NM - 1:
                @pl.when(q < NB)
                def _():
                    acopy(n + 1, b).wait()

                @pl.when(q + NA - 1 < NB)
                def _():
                    acopy(n + 1, b + NA - 1).start()

            if n < NM - 2:
                @pl.when(q + NA - 1 >= SM)
                def _():
                    acopy(n + 2, q + NA - 1 - SM).start()

            serve(s)
            if n < NM - 1:
                for i in range(8):
                    turn(later, b, i)
            rows = pl.ds(pl.multiple_of(r * TM, TM), TM)
            lhs = jnp.concatenate([now[k, rows, :] for k in range(KS)], axis=1)
            pb[lax.rem(s, NP)] = jnp.dot(lhs, gbuf[lax.rem(u, 2)], preferred_element_type=F32)
            stage_x(s)
            return 0

        lax.fori_loop(0, SM, step, 0)

    def drain(s, _):
        stage_x(s)
        serve(s)
        return 0

    lax.fori_loop(S, S + LH + NS, drain, 0)


def solution(mesh):
    dma = pltpu.SemaphoreType.DMA

    def sums(a, g):
        return pl.pallas_call(
            kernel,
            out_shape=jax.ShapeDtypeStruct((NM, D, F), BF16),
            in_specs=[pl.BlockSpec(memory_space=pltpu.HBM)] * 2,
            out_specs=pl.BlockSpec(memory_space=pltpu.HBM),
            scratch_shapes=[
                pltpu.VMEM((KS, D, 256), BF16),
                pltpu.VMEM((KS, D, 256), BF16),
                pltpu.VMEM((2, T, TN), BF16),
                pltpu.VMEM((NA, KB, D), BF16),
                pltpu.VMEM((NP, TM, TN), F32),
                pltpu.VMEM((NS, H, TN), BF16),
                pltpu.VMEM((NR, H, TN), BF16),
                pltpu.VMEM((NS, H, TN), BF16),
                pltpu.VMEM((NR, H, TN), BF16),
                pltpu.VMEM((NR, H, TN), BF16),
                pltpu.VMEM((NS, H, TN), BF16),
                dma((NA,)), dma((2,)),
                dma((NS,)), dma((NR,)),
                dma((NS,)), dma((NR,)), dma((NR,)),
                dma((NS, 4)), dma((NR,)), dma((NS, 2)), dma((NR,)),
            ],
            compiler_params=pltpu.CompilerParams(
                collective_id=1, has_side_effects=True, vmem_limit_bytes=67043328),
            name="sums",
        )(a, g)

    def step(a, g):
        return jax.shard_map(
            lambda a, g: sums(a[0], g[0]), mesh=mesh,
            in_specs=(P(("rep", "dp")), P(("rep", "dp"))), out_specs=P("rep"), check_vma=False)(a, g)

    return step
```

```python
import jax
import jax.numpy as jnp
from jax import lax
from jax.experimental import pallas as pl
from jax.experimental.pallas import tpu as pltpu
from jax.sharding import PartitionSpec as P

MESH = pl.DeviceIdType.MESH
BF16, F32 = jnp.bfloat16, jnp.float32

T, D, F, NM = 8192, 1024, 2816, 4
TM, TN = 512, 256
H = TM // 2
KT = 256
KS = T // KT
HB = TM // KT
KB = 512
NB = T // KB
KD = 8
NA = 2
NO = 4
R, J = D // TM, F // TN
SM = R * J
RUN = NM
S = RUN * SM
SX = (NM - 1) * SM
NX, NE, NM2 = 11, 10, 4
NF = 16
NP = 7
NS = 4
LX, LE, LM, LF, LG, LH = 2, 4, 6, 8, 10, 12


def kernel(a, g, x, o, at1, gbuf, araw, pb, xs, xr, es, er, mr, fs, hsem, asem, gsem,
           xss, xrs, ess, ers, mrs, fss, frs, gss, hrs, osem):
    me = lax.axis_index("dp")
    z, c = me // 2, lax.rem(me, 2)
    end = (z == 0) | (z == 3)
    mid = (z == 1) | (z == 2)

    def dev(zz, cc):
        return {"dp": zz * 2 + cc}

    z_mid = jnp.where(z == 0, 1, 2)
    z_end = jnp.where(z == 1, 0, 3)
    z_other = jnp.where(z == 1, 2, 1)
    inward = dev(jnp.where(end, z_mid, z_other), c)
    sibling = dev(z, 1 - c)

    def even(k, rows):
        return x.at[k // J, rows, pl.ds(pl.multiple_of(k % J * TN, TN), TN)]

    def odd(k, rows):
        return at1.at[k, rows, :]

    ats = (even, odd)

    def acopy(n, b):
        i = lax.rem(b, NA)
        return pltpu.make_async_copy(a.at[n, pl.ds(b * KB, KB), :], araw.at[i], asem.at[i])

    def gcopy(u):
        cols = pl.ds(pl.multiple_of(lax.rem(u, J) * TN, TN), TN)
        return pltpu.make_async_copy(g.at[u // J, :, cols], gbuf.at[lax.rem(u, 2)], gsem.at[lax.rem(u, 2)])

    def hcopy(i, k):
        rows = pl.ds(i * KT, KT)
        return pltpu.make_async_copy(a.at[0, pl.ds(k * KT, KT), rows], at1.at[k, rows, :], hsem.at[i, k])

    def dot(at, rows, gb):
        total = None
        for k in range(0, KS, KD):
            lhs = jnp.concatenate([at(i, rows)[...] for i in range(k, k + KD)], axis=1)
            term = jnp.dot(lhs, gb[pl.ds(k * KT, KD * KT), :], preferred_element_type=F32)
            total = term if total is None else total + term
        return total

    def remote(src, dst, send, recv, device):
        return pltpu.make_async_remote_copy(
            src_ref=src, dst_ref=dst, send_sem=send, recv_sem=recv, device_id=device, device_id_type=MESH)


    def xcopy(u):
        i, k = lax.rem(u, NX), lax.rem(u, 2)
        return remote(xs.at[k], xr.at[i], xss.at[k], xrs.at[i], sibling)

    def ecopy(u):
        i, k = lax.rem(u, NE), lax.rem(u, NS)
        return remote(es.at[k], er.at[i], ess.at[k], ers.at[i], inward)

    def mcopy(u):
        i, k = lax.rem(u // 2, NM2), lax.rem(u, NS)
        return remote(es.at[k], mr.at[i], ess.at[k], mrs.at[i], inward)

    def fcopies(u, at):
        i, k = lax.rem(u, NF), lax.rem(u, NS)
        return (
            remote(fs.at[k], at, fss.at[k, 0], frs.at[i], dev(z_end, c)),
            remote(fs.at[k], at, fss.at[k, 1], frs.at[i], dev(z_other, c)),
            remote(fs.at[k], at, fss.at[k, 2], hrs.at[i], sibling),
        )

    def fkeep(u, at):
        k = lax.rem(u, NS)
        return pltpu.make_async_copy(fs.at[k], at, fss.at[k, 3])

    def onward(u, at):
        i, k = lax.rem(u, NF), lax.rem(u, NS)
        return remote(at, at, gss.at[k, 0], frs.at[i], dev(z_end, c))

    def across(u, at):
        i, k = lax.rem(u, NF), lax.rem(u, NS)
        return remote(at, at, gss.at[k, 1], hrs.at[i], sibling)

    def placed(u, do):
        q = lax.rem(u, SM)
        rows = pl.ds(pl.multiple_of(lax.rem(q, R) * TM + c * H, H), H)
        cols = pl.ds(pl.multiple_of(q // R * TN, TN), TN)

        @pl.when(u < SX)
        def _():
            do(o.at[u // SM, rows, cols])

        @pl.when(u >= SX)
        def _():
            do(x.at[NM - 1, rows, cols])

    def mine(u):
        return z == 1 + lax.rem(u, 2)

    def chip_sum(u):
        return pb[lax.rem(u, NP), pl.ds(pl.multiple_of(c * H, H), H), :] + xr[lax.rem(u, NX)].astype(F32)

    def live(u):
        return (u >= 0) & (u < S)

    def stage_x(u):
        @pl.when(live(u - 2))
        def _():
            xcopy(u - 2).wait_send()

        @pl.when(live(u))
        def _():
            xs[lax.rem(u, 2)] = pb[lax.rem(u, NP), pl.ds(pl.multiple_of((1 - c) * H, H), H), :].astype(BF16)
            xcopy(u).start()

    def stage_end(u):
        @pl.when(end & live(u - NS))
        def _():
            ecopy(u - NS).wait_send()

        @pl.when(end & live(u))
        def _():
            xcopy(u).wait_recv()
            es[lax.rem(u, NS)] = chip_sum(u).astype(BF16)
            ecopy(u).start()

    def stage_pass(u):
        pass_on = mid & ~mine(u)

        @pl.when(pass_on & live(u - NS))
        def _():
            mcopy(u - NS).wait_send()

        @pl.when(pass_on & live(u))
        def _():
            xcopy(u).wait_recv()
            ecopy(u).wait_recv()
            es[lax.rem(u, NS)] = (chip_sum(u) + er[lax.rem(u, NE)].astype(F32)).astype(BF16)
            mcopy(u).start()

    def stage_own(u):
        k = lax.rem(u, NS)

        @pl.when(mid & mine(u) & live(u - NS))
        def _():
            for copy in fcopies(u - NS, er.at[0]):
                copy.wait_send()
            fkeep(u - NS, er.at[0]).wait()

        @pl.when(mid & mine(u) & live(u))
        def _():
            xcopy(u).wait_recv()
            ecopy(u).wait_recv()
            mcopy(u).wait_recv()
            fs[k] = (chip_sum(u) + er[lax.rem(u, NE)].astype(F32) + mr[lax.rem(u // 2, NM2)].astype(F32)).astype(BF16)

            def send(at):
                for copy in fcopies(u, at):
                    copy.start()
                fkeep(u, at).start()

            placed(u, send)

    def stage_forward(u):
        pass_on = mid & ~mine(u)

        @pl.when(pass_on & live(u - NS))
        def _():
            onward(u - NS, er.at[0]).wait_send()
            across(u - NS, er.at[0]).wait_send()

        @pl.when(pass_on & live(u))
        def _():
            onward(u, er.at[0]).wait_recv()

            def send(at):
                onward(u, at).start()
                across(u, at).start()

            placed(u, send)

    def stage_last(u):

        @pl.when(end & live(u - NS))
        def _():
            across(u - NS, er.at[0]).wait_send()

        @pl.when(end & live(u))
        def _():
            onward(u, er.at[0]).wait_recv()
            placed(u, lambda at: across(u, at).start())

    def stage_home(u):
        @pl.when(live(u))
        def _():
            across(u, er.at[0]).wait_recv()

    def serve(s):
        stage_end(s - LX)
        stage_own(s - LM)
        stage_forward(s - LF)
        stage_pass(s - LE)
        stage_last(s - LG)
        stage_home(s - LH)

    def take(p):
        cols = pl.ds(pl.multiple_of(lax.rem(p, J) * TN, TN), TN)
        at = (p // J, slice(None), cols)
        return pltpu.make_async_copy(o.at[at], x.at[at], osem.at[lax.rem(p, NO)])

    barrier = pltpu.get_barrier_semaphore()
    pl.semaphore_signal(barrier, inc=1, device_id=sibling, device_id_type=MESH)

    @pl.when(z > 0)
    def _():
        pl.semaphore_signal(barrier, inc=1, device_id=dev(z - 1, c), device_id_type=MESH)

    @pl.when(z < 3)
    def _():
        pl.semaphore_signal(barrier, inc=1, device_id=dev(z + 1, c), device_id_type=MESH)

    def fetch(r):
        def one(k, _):
            for i in range(r * HB, (r + 1) * HB):
                hcopy(i, k).start()
            return 0

        lax.fori_loop(0, KS, one, 0)

    def await_first(r, k):
        for i in range(r * HB, (r + 1) * HB):
            hcopy(i, k).wait()

    def turn_first(r, k):
        for i in range(r * HB, (r + 1) * HB):
            rows = pl.ds(i * KT, KT)
            even(k, rows)[...] = at1[k, rows, :].T

    fetch(0)
    gcopy(0).start()
    for r in range(1, R):
        fetch(r)
    for b in range(NA - 1 if RUN > 1 else 0):
        acopy(1, b).start()
    gcopy(1).start()

    def first(k, _):
        await_first(0, k)
        turn_first(0, k)
        return 0

    lax.fori_loop(0, KS, first, 0)

    @pl.when(end)
    def _():
        pl.semaphore_wait(barrier, 2)

    @pl.when(mid)
    def _():
        pl.semaphore_wait(barrier, 3)

    gcopy(0).wait()
    for r in range(R):
        serve(jnp.int32(r))
        if r < R - 1:
            for k in range(KS):
                await_first(r + 1, k)
            for k in range(KS):
                turn_first(r + 1, k)
        pb[r % NP] = dot(even, pl.ds(r * TM, TM), gbuf.at[0])
        stage_x(jnp.int32(r))

    for n in range(RUN):
        now, later = ats[n % 2], ats[(n + 1) % 2]

        def step(q, _, n=n, now=now, later=later):
            s = n * SM + q
            j, r = q // R, lax.rem(q, R)
            u = n * J + j

            @pl.when(r == 0)
            def _():
                gcopy(u).wait()

                @pl.when(u + 1 < RUN * J)
                def _():
                    gcopy(u + 1).start()

            q0 = R if n == 0 else 0
            b = jnp.minimum(q - q0, NB - 1)
            if n < RUN - 1:
                @pl.when(q - q0 < NB)
                def _():
                    acopy(n + 1, b).wait()

                @pl.when(q - q0 + NA - 1 < NB)
                def _():
                    acopy(n + 1, b + NA - 1).start()

            if n < RUN - 2:
                @pl.when(q + NA - 1 >= SM)
                def _():
                    acopy(n + 2, q + NA - 1 - SM).start()

            if n == NM - 1:
                for p in (2 * q, 2 * q + 1):
                    @pl.when((p >= NO) & (p - NO < SX // R))
                    def _(p=p):
                        take(p - NO).wait()

                    @pl.when(p < SX // R)
                    def _(p=p):
                        take(p).start()

            serve(s)
            if n < RUN - 1:
                for i in range(KB // KT):
                    for part in range(D // 256):
                        part = pl.ds(part * 256, 256)
                        later(b * (KB // KT) + i, part)[...] = araw[lax.rem(b, NA), pl.ds(i * KT, KT), part].T
            pb[lax.rem(s, NP)] = dot(now, pl.ds(pl.multiple_of(r * TM, TM), TM), gbuf.at[lax.rem(u, 2)])
            stage_x(s)
            return 0

        lax.fori_loop(R if n == 0 else 0, SM, step, 0)

    def drain(s, _):
        stage_x(s)
        serve(s)
        return 0

    lax.fori_loop(S, S + LH + NS, drain, 0)


def put(x, out, sem):
    copies = [pltpu.make_async_copy(x.at[n], out.at[n], sem.at[n]) for n in range(NM)]
    for copy in copies:
        copy.start()
    for copy in copies:
        copy.wait()


def solution(mesh):
    dma = pltpu.SemaphoreType.DMA

    def sums(a, g):
        x, _ = pl.pallas_call(
            kernel,
            out_shape=(pltpu.VMEM((NM, D, F), BF16), jax.ShapeDtypeStruct((NM - 1, D, F), BF16)),
            in_specs=[pl.BlockSpec(memory_space=pltpu.HBM)] * 2,
            out_specs=(pl.BlockSpec(memory_space=pltpu.VMEM), pl.BlockSpec(memory_space=pltpu.HBM)),
            scratch_shapes=[
                pltpu.VMEM((KS, D, KT), BF16),
                pltpu.VMEM((2, T, TN), BF16),
                pltpu.VMEM((NA, KB, D), BF16),
                pltpu.VMEM((NP, TM, TN), F32),
                pltpu.VMEM((2, H, TN), BF16),
                pltpu.VMEM((NX, H, TN), BF16),
                pltpu.VMEM((NS, H, TN), BF16),
                pltpu.VMEM((NE, H, TN), BF16),
                pltpu.VMEM((NM2, H, TN), BF16),
                pltpu.VMEM((NS, H, TN), BF16),
                dma((D // KT, KS)), dma((NA,)), dma((2,)),
                dma((2,)), dma((NX,)),
                dma((NS,)), dma((NE,)), dma((NM2,)),
                dma((NS, 4)), dma((NF,)), dma((NS, 2)), dma((NF,)), dma((NO,)),
            ],
            compiler_params=pltpu.CompilerParams(
                collective_id=1, has_side_effects=True, vmem_limit_bytes=43_900_000),
            name="sums",
        )(a, g)
        return pl.pallas_call(
            put,
            out_shape=jax.ShapeDtypeStruct((NM, D, F), BF16),
            in_specs=[pl.BlockSpec(memory_space=pltpu.VMEM)],
            out_specs=pl.BlockSpec(memory_space=pltpu.HBM),
            scratch_shapes=[dma((NM,))],
            compiler_params=pltpu.CompilerParams(vmem_limit_bytes=2**20),
            name="put",
        )(x)

    def step(a, g):
        return jax.shard_map(
            lambda a, g: sums(a[0], g[0]), mesh=mesh,
            in_specs=(P(("rep", "dp")), P(("rep", "dp"))), out_specs=P("rep"), check_vma=False)(a, g)

    return step
```

```python
import jax
import jax.numpy as jnp
from jax import lax
from jax.experimental import pallas as pl
from jax.experimental.pallas import tpu as pltpu
from jax.sharding import PartitionSpec as P

MESH = pl.DeviceIdType.MESH
BF16, F32 = jnp.bfloat16, jnp.float32

T, D, F, NM = 8192, 1024, 2816, 4
TM, TN = 512, 256
H = TM // 2
KT = 256
KS = T // KT
HB = TM // KT
HG = 4
KB = 512
NB = T // KB
KD = 8
NA = 2
NO = 4
R, J = D // TM, F // TN
SM = R * J
RUN = NM
S = RUN * SM
SX = (NM - 1) * SM
NX, NE, NM2 = 11, 10, 4
NF = 16
NP = 7
NS = 4
LX, LE, LM, LF, LG, LH = 2, 4, 6, 8, 10, 12


def kernel(a, g, x, o, at1, gbuf, araw, pb, xs, xr, es, er, mr, fs, hsem, asem, gsem,
           xss, xrs, ess, ers, mrs, fss, frs, gss, hrs, osem):
    me = lax.axis_index("dp")
    z, c = me // 2, lax.rem(me, 2)
    end = (z == 0) | (z == 3)
    mid = (z == 1) | (z == 2)

    def dev(zz, cc):
        return {"dp": zz * 2 + cc}

    z_mid = jnp.where(z == 0, 1, 2)
    z_end = jnp.where(z == 1, 0, 3)
    z_other = jnp.where(z == 1, 2, 1)
    inward = dev(jnp.where(end, z_mid, z_other), c)
    sibling = dev(z, 1 - c)

    def even(k, rows):
        return x.at[k // J, rows, pl.ds(pl.multiple_of(k % J * TN, TN), TN)]

    def odd(k, rows):
        return at1.at[pl.ds(pl.multiple_of(k * D + rows.start, KT), rows.size), :]

    ats = (even, odd)

    def acopy(n, b):
        i = lax.rem(b, NA)
        return pltpu.make_async_copy(a.at[n, pl.ds(b * KB, KB), :], araw.at[i], asem.at[i])

    def gcopy(u):
        cols = pl.ds(pl.multiple_of(lax.rem(u, J) * TN, TN), TN)
        return pltpu.make_async_copy(g.at[u // J, :, cols], gbuf.at[lax.rem(u, 2)], gsem.at[lax.rem(u, 2)])

    def hcopy(i, first, tokens, which):
        return pltpu.make_async_copy(
            a.at[0, pl.ds(first, tokens), pl.ds(i * KT, KT)], at1.at[pl.ds(i * T + first, tokens), :], hsem.at[which])

    def dot(at, rows, gb):
        total = None
        for k in range(0, KS, KD):
            lhs = jnp.concatenate([at(i, rows)[...] for i in range(k, k + KD)], axis=1)
            term = jnp.dot(lhs, gb[pl.ds(k * KT, KD * KT), :], preferred_element_type=F32)
            total = term if total is None else total + term
        return total

    def remote(src, dst, send, recv, device):
        return pltpu.make_async_remote_copy(
            src_ref=src, dst_ref=dst, send_sem=send, recv_sem=recv, device_id=device, device_id_type=MESH)


    def xcopy(u):
        i, k = lax.rem(u, NX), lax.rem(u, 2)
        return remote(xs.at[k], xr.at[i], xss.at[k], xrs.at[i], sibling)

    def ecopy(u):
        i, k = lax.rem(u, NE), lax.rem(u, NS)
        return remote(es.at[k], er.at[i], ess.at[k], ers.at[i], inward)

    def mcopy(u):
        i, k = lax.rem(u // 2, NM2), lax.rem(u, NS)
        return remote(es.at[k], mr.at[i], ess.at[k], mrs.at[i], inward)

    def fcopies(u, at):
        i, k = lax.rem(u, NF), lax.rem(u, NS)
        return (
            remote(fs.at[k], at, fss.at[k, 0], frs.at[i], dev(z_end, c)),
            remote(fs.at[k], at, fss.at[k, 1], frs.at[i], dev(z_other, c)),
            remote(fs.at[k], at, fss.at[k, 2], hrs.at[i], sibling),
        )

    def fkeep(u, at):
        k = lax.rem(u, NS)
        return pltpu.make_async_copy(fs.at[k], at, fss.at[k, 3])

    def onward(u, at):
        i, k = lax.rem(u, NF), lax.rem(u, NS)
        return remote(at, at, gss.at[k, 0], frs.at[i], dev(z_end, c))

    def across(u, at):
        i, k = lax.rem(u, NF), lax.rem(u, NS)
        return remote(at, at, gss.at[k, 1], hrs.at[i], sibling)

    def placed(u, do):
        q = lax.rem(u, SM)
        rows = pl.ds(pl.multiple_of(lax.rem(q, R) * TM + c * H, H), H)
        cols = pl.ds(pl.multiple_of(q // R * TN, TN), TN)

        @pl.when(u < SX)
        def _():
            do(o.at[u // SM, rows, cols])

        @pl.when(u >= SX)
        def _():
            do(x.at[NM - 1, rows, cols])

    def mine(u):
        return z == 1 + lax.rem(u, 2)

    def chip_sum(u):
        return pb[lax.rem(u, NP), pl.ds(pl.multiple_of(c * H, H), H), :] + xr[lax.rem(u, NX)].astype(F32)

    def live(u):
        return (u >= 0) & (u < S)

    def stage_x(u):
        @pl.when(live(u - 2))
        def _():
            xcopy(u - 2).wait_send()

        @pl.when(live(u))
        def _():
            xs[lax.rem(u, 2)] = pb[lax.rem(u, NP), pl.ds(pl.multiple_of((1 - c) * H, H), H), :].astype(BF16)
            xcopy(u).start()

    def stage_end(u):
        @pl.when(end & live(u - NS))
        def _():
            ecopy(u - NS).wait_send()

        @pl.when(end & live(u))
        def _():
            xcopy(u).wait_recv()
            es[lax.rem(u, NS)] = chip_sum(u).astype(BF16)
            ecopy(u).start()

    def stage_pass(u):
        pass_on = mid & ~mine(u)

        @pl.when(pass_on & live(u - NS))
        def _():
            mcopy(u - NS).wait_send()

        @pl.when(pass_on & live(u))
        def _():
            xcopy(u).wait_recv()
            ecopy(u).wait_recv()
            es[lax.rem(u, NS)] = (chip_sum(u) + er[lax.rem(u, NE)].astype(F32)).astype(BF16)
            mcopy(u).start()

    def stage_own(u):
        k = lax.rem(u, NS)

        @pl.when(mid & mine(u) & live(u - NS))
        def _():
            for copy in fcopies(u - NS, er.at[0]):
                copy.wait_send()
            fkeep(u - NS, er.at[0]).wait()

        @pl.when(mid & mine(u) & live(u))
        def _():
            xcopy(u).wait_recv()
            ecopy(u).wait_recv()
            mcopy(u).wait_recv()
            fs[k] = (chip_sum(u) + er[lax.rem(u, NE)].astype(F32) + mr[lax.rem(u // 2, NM2)].astype(F32)).astype(BF16)

            def send(at):
                for copy in fcopies(u, at):
                    copy.start()
                fkeep(u, at).start()

            placed(u, send)

    def stage_forward(u):
        pass_on = mid & ~mine(u)

        @pl.when(pass_on & live(u - NS))
        def _():
            onward(u - NS, er.at[0]).wait_send()
            across(u - NS, er.at[0]).wait_send()

        @pl.when(pass_on & live(u))
        def _():
            onward(u, er.at[0]).wait_recv()

            def send(at):
                onward(u, at).start()
                across(u, at).start()

            placed(u, send)

    def stage_last(u):

        @pl.when(end & live(u - NS))
        def _():
            across(u - NS, er.at[0]).wait_send()

        @pl.when(end & live(u))
        def _():
            onward(u, er.at[0]).wait_recv()
            placed(u, lambda at: across(u, at).start())

    def stage_home(u):
        @pl.when(live(u))
        def _():
            across(u, er.at[0]).wait_recv()

    def serve(s):
        stage_end(s - LX)
        stage_own(s - LM)
        stage_forward(s - LF)
        stage_pass(s - LE)
        stage_last(s - LG)
        stage_home(s - LH)

    def take(p):
        cols = pl.ds(pl.multiple_of(lax.rem(p, J) * TN, TN), TN)
        at = (p // J, slice(None), cols)
        return pltpu.make_async_copy(o.at[at], x.at[at], osem.at[lax.rem(p, NO)])

    barrier = pltpu.get_barrier_semaphore()
    pl.semaphore_signal(barrier, inc=1, device_id=sibling, device_id_type=MESH)

    @pl.when(z > 0)
    def _():
        pl.semaphore_signal(barrier, inc=1, device_id=dev(z - 1, c), device_id_type=MESH)

    @pl.when(z < 3)
    def _():
        pl.semaphore_signal(barrier, inc=1, device_id=dev(z + 1, c), device_id_type=MESH)

    def turn_first(i, k):
        rows = pl.ds(i * KT, KT)
        even(k, rows)[...] = at1[pl.ds(pl.multiple_of(i * T + k * KT, KT), KT), :].T

    HT = T // HG
    firsts = [hcopy(0, i * HT, HT, i) for i in range(HG)]
    for copy in firsts:
        copy.start()
    gcopy(0).start()
    parts = [None] + [hcopy(i, 0, T, HG - 1 + i) for i in range(1, D // KT)]
    for copy in parts[1:]:
        copy.start()
    for b in range(NA - 1 if RUN > 1 else 0):
        acopy(1, b).start()
    gcopy(1).start()
    for i, copy in enumerate(firsts):
        copy.wait()
        for k in range(i * KS // HG, (i + 1) * KS // HG):
            turn_first(0, k)

    @pl.when(end)
    def _():
        pl.semaphore_wait(barrier, 2)

    @pl.when(mid)
    def _():
        pl.semaphore_wait(barrier, 3)

    gcopy(0).wait()
    for i in range(D // KT):
        r, rows = i // HB, pl.ds(i % HB * KT, KT)
        if i % HB == 0:
            serve(jnp.int32(r))
        if i < D // KT - 1:
            parts[i + 1].wait()
            for k in range(KS):
                turn_first(i + 1, k)
        pb[r % NP, rows, :] = dot(even, pl.ds(i * KT, KT), gbuf.at[0])
        if i % HB == HB - 1:
            stage_x(jnp.int32(r))

    for n in range(RUN):
        now, later = ats[n % 2], ats[(n + 1) % 2]

        def step(q, _, n=n, now=now, later=later):
            s = n * SM + q
            j, r = q // R, lax.rem(q, R)
            u = n * J + j

            @pl.when(r == 0)
            def _():
                gcopy(u).wait()

                @pl.when(u + 1 < RUN * J)
                def _():
                    gcopy(u + 1).start()

            q0 = R if n == 0 else 0
            b = jnp.minimum(q - q0, NB - 1)
            if n < RUN - 1:
                @pl.when(q - q0 < NB)
                def _():
                    acopy(n + 1, b).wait()

                @pl.when(q - q0 + NA - 1 < NB)
                def _():
                    acopy(n + 1, b + NA - 1).start()

            if n < RUN - 2:
                @pl.when(q + NA - 1 >= SM)
                def _():
                    acopy(n + 2, q + NA - 1 - SM).start()

            if n == NM - 1:
                for p in (2 * q, 2 * q + 1):
                    @pl.when((p >= NO) & (p - NO < SX // R))
                    def _(p=p):
                        take(p - NO).wait()

                    @pl.when(p < SX // R)
                    def _(p=p):
                        take(p).start()

            serve(s)
            if n < RUN - 1:
                for i in range(KB // KT):
                    for part in range(D // 256):
                        part = pl.ds(part * 256, 256)
                        later(b * (KB // KT) + i, part)[...] = araw[lax.rem(b, NA), pl.ds(i * KT, KT), part].T
            pb[lax.rem(s, NP)] = dot(now, pl.ds(pl.multiple_of(r * TM, TM), TM), gbuf.at[lax.rem(u, 2)])
            stage_x(s)
            return 0

        lax.fori_loop(R if n == 0 else 0, SM, step, 0)

    def drain(s, _):
        stage_x(s)
        serve(s)
        return 0

    lax.fori_loop(S, S + LH + NS, drain, 0)


def put(x, out, sem):
    copies = [pltpu.make_async_copy(x.at[n], out.at[n], sem.at[n]) for n in range(NM)]
    for copy in copies:
        copy.start()
    for copy in copies:
        copy.wait()


def solution(mesh):
    dma = pltpu.SemaphoreType.DMA

    def sums(a, g):
        x, _ = pl.pallas_call(
            kernel,
            out_shape=(pltpu.VMEM((NM, D, F), BF16), jax.ShapeDtypeStruct((NM - 1, D, F), BF16)),
            in_specs=[pl.BlockSpec(memory_space=pltpu.HBM)] * 2,
            out_specs=(pl.BlockSpec(memory_space=pltpu.VMEM), pl.BlockSpec(memory_space=pltpu.HBM)),
            scratch_shapes=[
                pltpu.VMEM((KS * D, KT), BF16),
                pltpu.VMEM((2, T, TN), BF16),
                pltpu.VMEM((NA, KB, D), BF16),
                pltpu.VMEM((NP, TM, TN), F32),
                pltpu.VMEM((2, H, TN), BF16),
                pltpu.VMEM((NX, H, TN), BF16),
                pltpu.VMEM((NS, H, TN), BF16),
                pltpu.VMEM((NE, H, TN), BF16),
                pltpu.VMEM((NM2, H, TN), BF16),
                pltpu.VMEM((NS, H, TN), BF16),
                dma((HG + D // KT - 1,)), dma((NA,)), dma((2,)),
                dma((2,)), dma((NX,)),
                dma((NS,)), dma((NE,)), dma((NM2,)),
                dma((NS, 4)), dma((NF,)), dma((NS, 2)), dma((NF,)), dma((NO,)),
            ],
            compiler_params=pltpu.CompilerParams(
                collective_id=1, has_side_effects=True, vmem_limit_bytes=43_900_000),
            name="sums",
        )(a, g)
        return pl.pallas_call(
            put,
            out_shape=jax.ShapeDtypeStruct((NM, D, F), BF16),
            in_specs=[pl.BlockSpec(memory_space=pltpu.VMEM)],
            out_specs=pl.BlockSpec(memory_space=pltpu.HBM),
            scratch_shapes=[dma((NM,))],
            compiler_params=pltpu.CompilerParams(vmem_limit_bytes=2**20),
            name="put",
        )(x)

    def step(a, g):
        return jax.shard_map(
            lambda a, g: sums(a[0], g[0]), mesh=mesh,
            in_specs=(P(("rep", "dp")), P(("rep", "dp"))), out_specs=P("rep"), check_vma=False)(a, g)

    return step
```

```python
import jax
import jax.numpy as jnp
from jax import lax
from jax.experimental import pallas as pl
from jax.experimental.pallas import tpu as pltpu
from jax.sharding import PartitionSpec as P

MESH = pl.DeviceIdType.MESH
BF16, F32 = jnp.bfloat16, jnp.float32

T, D, F, NM = 8192, 1024, 2816, 4
TM, TN = 512, 256
H = TM // 2
KT = 256
KS = T // KT
HB = TM // KT
HG = 4
KB = 512
NB = T // KB
KD = 8
NA = 2
NO = 4
R, J = D // TM, F // TN
SM = R * J
RUN = NM
S = RUN * SM
SX = (NM - 1) * SM
NX, NE, NM2 = 11, 10, 8
NF = 16
NP = 7
NS = 4
NU = 2
HU = H // NU
LX, LE, LM, LF, LG, LH = 2, 3, 5, 7, 9, 11


def when(condition):
    if isinstance(condition, bool):
        return lambda do: do() if condition else None
    return pl.when(condition)


def kernel(a, g, x, o, at1, gbuf, araw, pb, xs, xr, es, er, mr, fs, hsem, asem, gsem,
           xss, xrs, ess, ers, mrs, fss, frs, gss, hrs, osem):
    me = lax.axis_index("dp")
    z, c = me // 2, lax.rem(me, 2)
    end = (z == 0) | (z == 3)
    mid = (z == 1) | (z == 2)

    def dev(zz, cc):
        return {"dp": zz * 2 + cc}

    z_mid = jnp.where(z == 0, 1, 2)
    z_end = jnp.where(z == 1, 0, 3)
    z_other = jnp.where(z == 1, 2, 1)
    inward = dev(jnp.where(end, z_mid, z_other), c)
    near = jnp.where(end, z_mid, z) - 1
    far = 1 - near
    sibling = dev(z, 1 - c)

    def even(k, rows):
        return x.at[k // J, rows, pl.ds(pl.multiple_of(k % J * TN, TN), TN)]

    def odd(k, rows):
        return at1.at[pl.ds(pl.multiple_of(k * D + rows.start, KT), rows.size), :]

    ats = (even, odd)

    def acopy(n, b):
        i = lax.rem(b, NA)
        return pltpu.make_async_copy(a.at[n, pl.ds(b * KB, KB), :], araw.at[i], asem.at[i])

    def gcopy(u):
        cols = pl.ds(pl.multiple_of(lax.rem(u, J) * TN, TN), TN)
        return pltpu.make_async_copy(g.at[u // J, :, cols], gbuf.at[lax.rem(u, 2)], gsem.at[lax.rem(u, 2)])

    def hcopy(i, first, tokens, which):
        return pltpu.make_async_copy(
            a.at[0, pl.ds(first, tokens), pl.ds(i * KT, KT)], at1.at[pl.ds(i * T + first, tokens), :], hsem.at[which])

    def dot(at, rows, gb):
        total = None
        for k in range(0, KS, KD):
            lhs = jnp.concatenate([at(i, rows)[...] for i in range(k, k + KD)], axis=1)
            term = jnp.dot(lhs, gb[pl.ds(k * KT, KD * KT), :], preferred_element_type=F32)
            total = term if total is None else total + term
        return total

    def remote(src, dst, send, recv, device):
        return pltpu.make_async_remote_copy(
            src_ref=src, dst_ref=dst, send_sem=send, recv_sem=recv, device_id=device, device_id_type=MESH)


    def xcopy(u):
        i, k = lax.rem(u, NX), lax.rem(u, 2)
        return remote(xs.at[k], xr.at[i], xss.at[k], xrs.at[i], sibling)

    def part(p):
        return pl.ds(pl.multiple_of(p * HU, HU), HU)

    def ecopy(u, p):
        i, k = lax.rem(u, NE), lax.rem(u, NS)
        return remote(es.at[k, part(p)], er.at[i, part(p)], ess.at[k, p], ers.at[i, p], inward)

    def mcopy(u):
        i, k = lax.rem(u, NM2), lax.rem(u, NS)
        return remote(es.at[k, part(far)], mr.at[i], ess.at[k, far], mrs.at[i], inward)

    def fcopies(u, p, at):
        i, k = lax.rem(u, NF), lax.rem(u, NS)
        src = fs.at[k]
        return (
            remote(src, at, fss.at[k, 0], frs.at[i, p], dev(z_end, c)),
            remote(src, at, fss.at[k, 1], frs.at[i, p], dev(z_other, c)),
            remote(src, at, fss.at[k, 2], hrs.at[i, p], sibling),
        )

    def fkeep(u, at):
        k = lax.rem(u, NS)
        return pltpu.make_async_copy(fs.at[k], at, fss.at[k, 3])

    def onward(u, p, at):
        i, k = lax.rem(u, NF), lax.rem(u, NS)
        return remote(at, at, gss.at[k, p, 0], frs.at[i, p], dev(z_end, c))

    def across(u, p, at):
        i, k = lax.rem(u, NF), lax.rem(u, NS)
        return remote(at, at, gss.at[k, p, 1], hrs.at[i, p], sibling)

    some = er.at[0, pl.ds(0, HU)]

    def placed(u, p, early, do):
        q = lax.rem(u, SM)
        rows = pl.ds(pl.multiple_of(lax.rem(q, R) * TM + c * H + p * HU, HU), HU)
        cols = pl.ds(pl.multiple_of(q // R * TN, TN), TN)

        @when(u < SX if early is None else early)
        def _():
            do(o.at[u // SM, rows, cols])

        @when(u >= SX if early is None else not early)
        def _():
            do(x.at[NM - 1, rows, cols])

    def chip_sum(u, p):
        own = pb[lax.rem(u, NP), pl.ds(pl.multiple_of(c * H + p * HU, HU), HU), :]
        return own + xr[lax.rem(u, NX), part(p), :].astype(F32)

    def live(u):
        return (u >= 0) & (u < S)

    def stage_x(u):
        @pl.when(live(u - 2))
        def _():
            xcopy(u - 2).wait_send()

        @pl.when(live(u))
        def _():
            xs[lax.rem(u, 2)] = pb[lax.rem(u, NP), pl.ds(pl.multiple_of((1 - c) * H, H), H), :].astype(BF16)
            xcopy(u).start()

    def stage_end(u, sure):
        @when(sure or live(u - NS))
        def _():
            for p in (far, near):
                ecopy(u - NS, p).wait_send()

        @when(sure or live(u))
        def _():
            xcopy(u).wait_recv()
            for p in (far, near):
                es[lax.rem(u, NS), part(p), :] = chip_sum(u, p).astype(BF16)
                ecopy(u, p).start()

    def stage_pass(u, sure):
        @when(sure or live(u - NS))
        def _():
            mcopy(u - NS).wait_send()

        @when(sure or live(u))
        def _():
            xcopy(u).wait_recv()
            ecopy(u, far).wait_recv()
            es[lax.rem(u, NS), part(far), :] = (
                chip_sum(u, far) + er[lax.rem(u, NE), part(far), :].astype(F32)).astype(BF16)
            mcopy(u).start()

    def stage_own(u, sure, early):
        @when(sure or live(u - NS))
        def _():
            for copy in fcopies(u - NS, near, some):
                copy.wait_send()
            fkeep(u - NS, some).wait()

        @when(sure or live(u))
        def _():
            ecopy(u, near).wait_recv()
            mcopy(u).wait_recv()
            chips = chip_sum(u, near) + er[lax.rem(u, NE), part(near), :].astype(F32)
            fs[lax.rem(u, NS)] = (chips + mr[lax.rem(u, NM2)].astype(F32)).astype(BF16)

            def send(at):
                for copy in fcopies(u, near, at):
                    copy.start()
                fkeep(u, at).start()

            placed(u, near, early, send)

    def stage_forward(u, sure, early):
        @when(sure or live(u - NS))
        def _():
            onward(u - NS, far, some).wait_send()
            across(u - NS, far, some).wait_send()

        @when(sure or live(u))
        def _():
            onward(u, far, some).wait_recv()

            def send(at):
                onward(u, far, at).start()
                across(u, far, at).start()

            placed(u, far, early, send)

    def stage_last(u, sure, early):
        @when(sure or live(u - NS))
        def _():
            for p in (near, far):
                across(u - NS, p, some).wait_send()

        @when(sure or live(u))
        def _():
            for p in (near, far):
                onward(u, p, some).wait_recv()
                placed(u, p, early, lambda at, p=p: across(u, p, at).start())

    def stage_home(u, sure):
        @when(sure or live(u))
        def _():
            for p in range(NU):
                across(u, p, some).wait_recv()

    def serve(s, sure=False, early=None):
        @pl.when(end)
        def _():
            stage_end(s - LX, sure)
            stage_last(s - LG, sure, early)

        @pl.when(mid)
        def _():
            stage_own(s - LM, sure, early)
            stage_forward(s - LF, sure, early)
            stage_pass(s - LE, sure)

        stage_home(s - LH, sure)

    def take(p):
        cols = pl.ds(pl.multiple_of(lax.rem(p, J) * TN, TN), TN)
        at = (p // J, slice(None), cols)
        return pltpu.make_async_copy(o.at[at], x.at[at], osem.at[lax.rem(p, NO)])

    barrier = pltpu.get_barrier_semaphore()
    pl.semaphore_signal(barrier, inc=1, device_id=sibling, device_id_type=MESH)

    @pl.when(z > 0)
    def _():
        pl.semaphore_signal(barrier, inc=1, device_id=dev(z - 1, c), device_id_type=MESH)

    @pl.when(z < 3)
    def _():
        pl.semaphore_signal(barrier, inc=1, device_id=dev(z + 1, c), device_id_type=MESH)

    def turn_first(i, k):
        rows = pl.ds(i * KT, KT)
        even(k, rows)[...] = at1[pl.ds(pl.multiple_of(i * T + k * KT, KT), KT), :].T

    HT = T // HG
    firsts = [hcopy(0, i * HT, HT, i) for i in range(HG)]
    for copy in firsts:
        copy.start()
    gcopy(0).start()
    parts = [None] + [hcopy(i, 0, T, HG - 1 + i) for i in range(1, D // KT)]
    for copy in parts[1:]:
        copy.start()
    for b in range(NA - 1 if RUN > 1 else 0):
        acopy(1, b).start()
    gcopy(1).start()
    for i, copy in enumerate(firsts):
        copy.wait()
        for k in range(i * KS // HG, (i + 1) * KS // HG):
            turn_first(0, k)

    @pl.when(end)
    def _():
        pl.semaphore_wait(barrier, 2)

    @pl.when(mid)
    def _():
        pl.semaphore_wait(barrier, 3)

    gcopy(0).wait()
    for i in range(D // KT):
        r, rows = i // HB, pl.ds(i % HB * KT, KT)
        if i % HB == 0:
            serve(jnp.int32(r), early=True)
        if i < D // KT - 1:
            parts[i + 1].wait()
            for k in range(KS):
                turn_first(i + 1, k)
        pb[r % NP, rows, :] = dot(even, pl.ds(i * KT, KT), gbuf.at[0])
        if i % HB == HB - 1:
            stage_x(jnp.int32(r))

    for n in range(RUN):
        now, later = ats[n % 2], ats[(n + 1) % 2]

        def step(q, _, n=n, now=now, later=later):
            s = n * SM + q
            j, r = q // R, lax.rem(q, R)
            u = n * J + j

            @pl.when(r == 0)
            def _():
                gcopy(u).wait()

                @pl.when(u + 1 < RUN * J)
                def _():
                    gcopy(u + 1).start()

            q0 = R if n == 0 else 0
            b = jnp.minimum(q - q0, NB - 1)
            if n < RUN - 1:
                @pl.when(q - q0 < NB)
                def _():
                    acopy(n + 1, b).wait()

                @pl.when(q - q0 + NA - 1 < NB)
                def _():
                    acopy(n + 1, b + NA - 1).start()

            if n < RUN - 2:
                @pl.when(q + NA - 1 >= SM)
                def _():
                    acopy(n + 2, q + NA - 1 - SM).start()

            if n == NM - 1:
                for p in (2 * q, 2 * q + 1):
                    @pl.when((p >= NO) & (p - NO < SX // R))
                    def _(p=p):
                        take(p - NO).wait()

                    @pl.when(p < SX // R)
                    def _(p=p):
                        take(p).start()

            serve(s, n > 0, True if n < NM - 1 else None)
            if n < RUN - 1:
                for i in range(KB // KT):
                    for part in range(D // 256):
                        part = pl.ds(part * 256, 256)
                        later(b * (KB // KT) + i, part)[...] = araw[lax.rem(b, NA), pl.ds(i * KT, KT), part].T
            pb[lax.rem(s, NP)] = dot(now, pl.ds(pl.multiple_of(r * TM, TM), TM), gbuf.at[lax.rem(u, 2)])
            stage_x(s)
            return 0

        lax.fori_loop(R if n == 0 else 0, SM, step, 0)

    def drain(s, _):
        stage_x(s)
        serve(s, early=SX >= S)
        return 0

    lax.fori_loop(S, S + LH + NS, drain, 0)


def put(x, out, sem):
    copies = [pltpu.make_async_copy(x.at[n], out.at[n], sem.at[n]) for n in range(NM)]
    for copy in copies:
        copy.start()
    for copy in copies:
        copy.wait()


def solution(mesh):
    dma = pltpu.SemaphoreType.DMA

    def sums(a, g):
        x, _ = pl.pallas_call(
            kernel,
            out_shape=(pltpu.VMEM((NM, D, F), BF16), jax.ShapeDtypeStruct((NM - 1, D, F), BF16)),
            in_specs=[pl.BlockSpec(memory_space=pltpu.HBM)] * 2,
            out_specs=(pl.BlockSpec(memory_space=pltpu.VMEM), pl.BlockSpec(memory_space=pltpu.HBM)),
            scratch_shapes=[
                pltpu.VMEM((KS * D, KT), BF16),
                pltpu.VMEM((2, T, TN), BF16),
                pltpu.VMEM((NA, KB, D), BF16),
                pltpu.VMEM((NP, TM, TN), F32),
                pltpu.VMEM((2, H, TN), BF16),
                pltpu.VMEM((NX, H, TN), BF16),
                pltpu.VMEM((NS, H, TN), BF16),
                pltpu.VMEM((NE, H, TN), BF16),
                pltpu.VMEM((NM2, HU, TN), BF16),
                pltpu.VMEM((NS, HU, TN), BF16),
                dma((HG + D // KT - 1,)), dma((NA,)), dma((2,)),
                dma((2,)), dma((NX,)),
                dma((NS, NU)), dma((NE, NU)), dma((NM2,)),
                dma((NS, 4)), dma((NF, NU)), dma((NS, NU, 2)), dma((NF, NU)), dma((NO,)),
            ],
            compiler_params=pltpu.CompilerParams(
                collective_id=1, has_side_effects=True, vmem_limit_bytes=43_900_000),
            name="sums",
        )(a, g)
        return pl.pallas_call(
            put,
            out_shape=jax.ShapeDtypeStruct((NM, D, F), BF16),
            in_specs=[pl.BlockSpec(memory_space=pltpu.VMEM)],
            out_specs=pl.BlockSpec(memory_space=pltpu.HBM),
            scratch_shapes=[dma((NM,))],
            compiler_params=pltpu.CompilerParams(vmem_limit_bytes=2**20),
            name="put",
        )(x)

    def step(a, g):
        return jax.shard_map(
            lambda a, g: sums(a[0], g[0]), mesh=mesh,
            in_specs=(P(("rep", "dp")), P(("rep", "dp"))), out_specs=P("rep"), check_vma=False)(a, g)

    return step
```

```python
import jax
import jax.numpy as jnp
from jax import lax
from jax.experimental import pallas as pl
from jax.experimental.pallas import tpu as pltpu
from jax.sharding import PartitionSpec as P

MESH = pl.DeviceIdType.MESH
BF16, F32 = jnp.bfloat16, jnp.float32

T, D, F, NM = 8192, 1024, 2816, 4
TM, TN = 512, 256
H = TM // 2
KT = 256
KS = T // KT
HB = TM // KT
HG = 4
KB = 512
NB = T // KB
KD = 8
NA = 2
NO = 4
R, J = D // TM, F // TN
SM = R * J
RUN = NM
S = RUN * SM
SX = (NM - 1) * SM
NX, NE, NM2 = 11, 10, 8
NF = 16
NP = 7
NS = 4
NU = 2
HU = H // NU
LX, LE, LM, LF, LG, LH = 2, 3, 5, 7, 9, 11


def when(condition):
    if isinstance(condition, bool):
        return lambda do: do() if condition else None
    return pl.when(condition)


def kernel(a, g, x, o, at1, gbuf, araw, pb, xs, xr, es, er, mr, fs, hsem, asem, gsem,
           xss, xrs, ess, ers, mrs, fss, frs, gss, hrs, osem):
    me = lax.axis_index("dp")
    z, c = me // 2, lax.rem(me, 2)
    end = (z == 0) | (z == 3)
    mid = (z == 1) | (z == 2)

    def dev(zz, cc):
        return {"dp": zz * 2 + cc}

    z_mid = jnp.where(z == 0, 1, 2)
    z_end = jnp.where(z == 1, 0, 3)
    z_other = jnp.where(z == 1, 2, 1)
    inward = dev(jnp.where(end, z_mid, z_other), c)
    near = jnp.where(end, z_mid, z) - 1
    far = 1 - near
    sibling = dev(z, 1 - c)

    def even(k, rows):
        return x.at[k // J, rows, pl.ds(pl.multiple_of(k % J * TN, TN), TN)]

    def odd(k, rows):
        return at1.at[pl.ds(pl.multiple_of(k * D + rows.start, KT), rows.size), :]

    ats = (even, odd)

    def acopy(n, b):
        i = lax.rem(b, NA)
        return pltpu.make_async_copy(a.at[n, pl.ds(b * KB, KB), :], araw.at[i], asem.at[i])

    def gcopy(u):
        cols = pl.ds(pl.multiple_of(lax.rem(u, J) * TN, TN), TN)
        return pltpu.make_async_copy(g.at[u // J, :, cols], gbuf.at[lax.rem(u, 2)], gsem.at[lax.rem(u, 2)])

    def hcopy(i, first, tokens, which):
        return pltpu.make_async_copy(
            a.at[0, pl.ds(first, tokens), pl.ds(i * KT, KT)], at1.at[pl.ds(i * T + first, tokens), :], hsem.at[which])

    def dot(at, rows, gb):
        total = None
        for k in range(0, KS, KD):
            lhs = jnp.concatenate([at(i, rows)[...] for i in range(k, k + KD)], axis=1)
            term = jnp.dot(lhs, gb[pl.ds(k * KT, KD * KT), :], preferred_element_type=F32)
            total = term if total is None else total + term
        return total

    def remote(src, dst, send, recv, device):
        return pltpu.make_async_remote_copy(
            src_ref=src, dst_ref=dst, send_sem=send, recv_sem=recv, device_id=device, device_id_type=MESH)


    def xcopy(u):
        i, k = lax.rem(u, NX), lax.rem(u, 2)
        return remote(xs.at[k], xr.at[i], xss.at[k], xrs.at[i], sibling)

    def part(p):
        return pl.ds(pl.multiple_of(p * HU, HU), HU)

    def ecopy(u, p):
        i, k = lax.rem(u, NE), lax.rem(u, NS)
        return remote(es.at[k, part(p)], er.at[i, part(p)], ess.at[k, p], ers.at[i, p], inward)

    def mcopy(u):
        i, k = lax.rem(u, NM2), lax.rem(u, NS)
        return remote(es.at[k, part(far)], mr.at[i], ess.at[k, far], mrs.at[i], inward)

    def fcopies(u, p, at):
        i, k = lax.rem(u, NF), lax.rem(u, NS)
        src = fs.at[k]
        return (
            remote(src, at, fss.at[k, 0], frs.at[i, p], dev(z_end, c)),
            remote(src, at, fss.at[k, 1], frs.at[i, p], dev(z_other, c)),
            remote(src, at, fss.at[k, 2], hrs.at[i, p], sibling),
        )

    def fkeep(u, at):
        k = lax.rem(u, NS)
        return pltpu.make_async_copy(fs.at[k], at, fss.at[k, 3])

    def onward(u, p, at):
        i, k = lax.rem(u, NF), lax.rem(u, NS)
        return remote(at, at, gss.at[k, p, 0], frs.at[i, p], dev(z_end, c))

    def across(u, p, at):
        i, k = lax.rem(u, NF), lax.rem(u, NS)
        return remote(at, at, gss.at[k, p, 1], hrs.at[i, p], sibling)

    some = er.at[0, pl.ds(0, HU)]

    def placed(u, p, early, do):
        q = lax.rem(u, SM)
        rows = pl.ds(pl.multiple_of(lax.rem(q, R) * TM + c * H + p * HU, HU), HU)
        cols = pl.ds(pl.multiple_of(q // R * TN, TN), TN)

        @when(u < SX if early is None else early)
        def _():
            do(o.at[u // SM, rows, cols])

        @when(u >= SX if early is None else not early)
        def _():
            do(x.at[NM - 1, rows, cols])

    def chip_sum(u, p):
        own = pb[lax.rem(u, NP), pl.ds(pl.multiple_of(c * H + p * HU, HU), HU), :]
        return own + xr[lax.rem(u, NX), part(p), :].astype(F32)

    def live(u):
        return (u >= 0) & (u < S)

    def stage_x(u):
        @pl.when(live(u - 2))
        def _():
            xcopy(u - 2).wait_send()

        @pl.when(live(u))
        def _():
            xs[lax.rem(u, 2)] = pb[lax.rem(u, NP), pl.ds(pl.multiple_of((1 - c) * H, H), H), :].astype(BF16)
            xcopy(u).start()

    def end_sum(u):
        xcopy(u).wait_recv()
        for p in (far, near):
            es[lax.rem(u, NS), part(p), :] = chip_sum(u, p).astype(BF16)
            ecopy(u, p).start()

    def stage_end(u, sure):
        @when(sure or live(u - NS))
        def _():
            for p in (far, near):
                ecopy(u - NS, p).wait_send()

        @when(sure or live(u) & (u > 0))
        def _():
            end_sum(u)

    def stage_pass(u, sure):
        @when(sure or live(u - NS))
        def _():
            mcopy(u - NS).wait_send()

        @when(sure or live(u))
        def _():
            xcopy(u).wait_recv()
            ecopy(u, far).wait_recv()
            es[lax.rem(u, NS), part(far), :] = (
                chip_sum(u, far) + er[lax.rem(u, NE), part(far), :].astype(F32)).astype(BF16)
            mcopy(u).start()

    def stage_own(u, sure, early):
        @when(sure or live(u - NS))
        def _():
            for copy in fcopies(u - NS, near, some):
                copy.wait_send()
            fkeep(u - NS, some).wait()

        @when(sure or live(u))
        def _():
            ecopy(u, near).wait_recv()
            mcopy(u).wait_recv()
            chips = chip_sum(u, near) + er[lax.rem(u, NE), part(near), :].astype(F32)
            fs[lax.rem(u, NS)] = (chips + mr[lax.rem(u, NM2)].astype(F32)).astype(BF16)

            def send(at):
                for copy in fcopies(u, near, at):
                    copy.start()
                fkeep(u, at).start()

            placed(u, near, early, send)

    def stage_forward(u, sure, early):
        @when(sure or live(u - NS))
        def _():
            onward(u - NS, far, some).wait_send()
            across(u - NS, far, some).wait_send()

        @when(sure or live(u))
        def _():
            onward(u, far, some).wait_recv()

            def send(at):
                onward(u, far, at).start()
                across(u, far, at).start()

            placed(u, far, early, send)

    def stage_last(u, sure, early):
        @when(sure or live(u - NS))
        def _():
            for p in (near, far):
                across(u - NS, p, some).wait_send()

        @when(sure or live(u))
        def _():
            for p in (near, far):
                onward(u, p, some).wait_recv()
                placed(u, p, early, lambda at, p=p: across(u, p, at).start())

    def stage_home(u, sure):
        @when(sure or live(u))
        def _():
            for p in range(NU):
                across(u, p, some).wait_recv()

    def serve(s, sure=False, early=None):
        @pl.when(end)
        def _():
            stage_end(s - LX, sure)
            stage_last(s - LG, sure, early)

        @pl.when(mid)
        def _():
            stage_own(s - LM, sure, early)
            stage_forward(s - LF, sure, early)
            stage_pass(s - LE, sure)

        stage_home(s - LH, sure)

    def take(p):
        cols = pl.ds(pl.multiple_of(lax.rem(p, J) * TN, TN), TN)
        at = (p // J, slice(None), cols)
        return pltpu.make_async_copy(o.at[at], x.at[at], osem.at[lax.rem(p, NO)])

    barrier = pltpu.get_barrier_semaphore()
    pl.semaphore_signal(barrier, inc=1, device_id=sibling, device_id_type=MESH)

    @pl.when(z > 0)
    def _():
        pl.semaphore_signal(barrier, inc=1, device_id=dev(z - 1, c), device_id_type=MESH)

    @pl.when(z < 3)
    def _():
        pl.semaphore_signal(barrier, inc=1, device_id=dev(z + 1, c), device_id_type=MESH)

    def turn_first(i, k):
        rows = pl.ds(i * KT, KT)
        even(k, rows)[...] = at1[pl.ds(pl.multiple_of(i * T + k * KT, KT), KT), :].T

    HT = T // HG
    firsts = [hcopy(0, i * HT, HT, i) for i in range(HG)]
    for copy in firsts:
        copy.start()
    gcopy(0).start()
    parts = [None] + [hcopy(i, 0, T, HG - 1 + i) for i in range(1, D // KT)]
    for copy in parts[1:]:
        copy.start()
    for b in range(NA - 1 if RUN > 1 else 0):
        acopy(1, b).start()
    gcopy(1).start()
    for i, copy in enumerate(firsts):
        copy.wait()
        for k in range(i * KS // HG, (i + 1) * KS // HG):
            turn_first(0, k)

    @pl.when(end)
    def _():
        pl.semaphore_wait(barrier, 2)

    @pl.when(mid)
    def _():
        pl.semaphore_wait(barrier, 3)

    gcopy(0).wait()
    for i in range(D // KT):
        r, rows = i // HB, pl.ds(i % HB * KT, KT)
        if i % HB == 0:
            serve(jnp.int32(r), early=True)
        if i < D // KT - 1:
            parts[i + 1].wait()
            for k in range(KS):
                turn_first(i + 1, k)
        else:
            @pl.when(end)
            def _():
                end_sum(jnp.int32(0))

        pb[r % NP, rows, :] = dot(even, pl.ds(i * KT, KT), gbuf.at[0])
        if i % HB == HB - 1:
            stage_x(jnp.int32(r))

    for n in range(RUN):
        now, later = ats[n % 2], ats[(n + 1) % 2]

        def step(q, _, n=n, now=now, later=later):
            s = n * SM + q
            j, r = q // R, lax.rem(q, R)
            u = n * J + j

            @pl.when(r == 0)
            def _():
                gcopy(u).wait()

                @pl.when(u + 1 < RUN * J)
                def _():
                    gcopy(u + 1).start()

            q0 = R if n == 0 else 0
            b = jnp.minimum(q - q0, NB - 1)
            if n < RUN - 1:
                @pl.when(q - q0 < NB)
                def _():
                    acopy(n + 1, b).wait()

                @pl.when(q - q0 + NA - 1 < NB)
                def _():
                    acopy(n + 1, b + NA - 1).start()

            if n < RUN - 2:
                @pl.when(q + NA - 1 >= SM)
                def _():
                    acopy(n + 2, q + NA - 1 - SM).start()

            if n == NM - 1:
                for p in (2 * q, 2 * q + 1):
                    @pl.when((p >= NO) & (p - NO < SX // R))
                    def _(p=p):
                        take(p - NO).wait()

                    @pl.when(p < SX // R)
                    def _(p=p):
                        take(p).start()

            serve(s, n > 0, True if n < NM - 1 else None)
            if n < RUN - 1:
                for i in range(KB // KT):
                    for part in range(D // 256):
                        part = pl.ds(part * 256, 256)
                        later(b * (KB // KT) + i, part)[...] = araw[lax.rem(b, NA), pl.ds(i * KT, KT), part].T
            pb[lax.rem(s, NP)] = dot(now, pl.ds(pl.multiple_of(r * TM, TM), TM), gbuf.at[lax.rem(u, 2)])
            stage_x(s)
            return 0

        lax.fori_loop(R if n == 0 else 0, SM, step, 0)

    def drain(s, _):
        stage_x(s)
        serve(s, early=SX >= S)
        return 0

    lax.fori_loop(S, S + LH + NS, drain, 0)


def put(x, out, sem):
    copies = [pltpu.make_async_copy(x.at[n], out.at[n], sem.at[n]) for n in range(NM)]
    for copy in copies:
        copy.start()
    for copy in copies:
        copy.wait()


def solution(mesh):
    dma = pltpu.SemaphoreType.DMA

    def sums(a, g):
        x, _ = pl.pallas_call(
            kernel,
            out_shape=(pltpu.VMEM((NM, D, F), BF16), jax.ShapeDtypeStruct((NM - 1, D, F), BF16)),
            in_specs=[pl.BlockSpec(memory_space=pltpu.HBM)] * 2,
            out_specs=(pl.BlockSpec(memory_space=pltpu.VMEM), pl.BlockSpec(memory_space=pltpu.HBM)),
            scratch_shapes=[
                pltpu.VMEM((KS * D, KT), BF16),
                pltpu.VMEM((2, T, TN), BF16),
                pltpu.VMEM((NA, KB, D), BF16),
                pltpu.VMEM((NP, TM, TN), F32),
                pltpu.VMEM((2, H, TN), BF16),
                pltpu.VMEM((NX, H, TN), BF16),
                pltpu.VMEM((NS, H, TN), BF16),
                pltpu.VMEM((NE, H, TN), BF16),
                pltpu.VMEM((NM2, HU, TN), BF16),
                pltpu.VMEM((NS, HU, TN), BF16),
                dma((HG + D // KT - 1,)), dma((NA,)), dma((2,)),
                dma((2,)), dma((NX,)),
                dma((NS, NU)), dma((NE, NU)), dma((NM2,)),
                dma((NS, 4)), dma((NF, NU)), dma((NS, NU, 2)), dma((NF, NU)), dma((NO,)),
            ],
            compiler_params=pltpu.CompilerParams(
                collective_id=1, has_side_effects=True, vmem_limit_bytes=43_900_000),
            name="sums",
        )(a, g)
        return pl.pallas_call(
            put,
            out_shape=jax.ShapeDtypeStruct((NM, D, F), BF16),
            in_specs=[pl.BlockSpec(memory_space=pltpu.VMEM)],
            out_specs=pl.BlockSpec(memory_space=pltpu.HBM),
            scratch_shapes=[dma((NM,))],
            compiler_params=pltpu.CompilerParams(vmem_limit_bytes=2**20),
            name="put",
        )(x)

    def step(a, g):
        return jax.shard_map(
            lambda a, g: sums(a[0], g[0]), mesh=mesh,
            in_specs=(P(("rep", "dp")), P(("rep", "dp"))), out_specs=P("rep"), check_vma=False)(a, g)

    return step
```
